32 devices in a mesh: subj: 2 (over y), row: 4 (over x, core), col: 4 (over z).
Axes of the slice: x: 2, y: 2, z: 4, core: 2. Of those that a mesh axis runs over, the one named last changes fastest.
Arguments:
- series: float32 [800, 4096], P(None, ('subj', 'row', 'col')), parts along dimension 1, as said below
- keep_mask: int32 [32, 16], P(('subj', 'row'), 'col'), parts along dimension 0, may hold values from 0 to 1, as said below
- row_owner: int32 [32], P('subj'), parts along dimension 0, may hold values from 0 to 3, as said below
Outputs:
- owned_tiles: bfloat16 [8, 4, 8, 128, 128], P(('subj', 'row'), 'col'), parts along dimension 0
- owned_ids: int32 [8, 4, 8], P(('subj', 'row'), 'col'), parts along dimension 0
The draws below stay inside these ranges and needn't reach their ends.
There are 2 independent parts, one for each index of `subj`. The reference program is written for one: setup_inputs(seed, part) draws one part's arguments, and reference() takes and returns one part's arrays. A program takes and returns all parts, laid end to end along the dimension named above; each array names one. Nothing has to cross between parts.
Inputs may be any that keep to these rules, and one draw needn't show every extreme that they name: Each voxel's series varies over time. `keep_mask`: of the 4 tiles that one tile row has in one column block, at most 2 are kept; in every draw one owner keeps exactly 2 in each of its tile rows in some column block. `row_owner`: the 4 tile rows of a row block have 4 different owners, and every owner holds 4 tile rows, from 4 different row blocks.
All inputs are finite; a program needn't handle non-finite values.
Results may differ from the reference program's by a relative error of at most 0.0042.
Values may be sent and summed in bfloat16 or wider, within the bound.
A program may use at most 64 MiB of HBM per device.

```python
import math
import jax
import jax.numpy as jnp
from jax import lax

TRS = 800
TILE = 128
CH = 128
NVOX = 2048
NTILES = 16
RT = 4
CT = 4
CAP = 2
RCAP = 8
N_ROW = 4
N_COL = 4


latent_count = 128


def draw_series(key, part):
    subkeys = jax.random.split(key, 6)
    latent = jax.random.normal(subkeys[0], (TRS, latent_count), jnp.float32)
    loadings = 1.2 / math.sqrt(latent_count) * jax.random.normal(subkeys[1], (latent_count, NVOX), jnp.float32)
    tr_scale = jnp.exp(jax.random.uniform(subkeys[4], (TRS, 1), jnp.float32, 0.0, math.log(1.2)))
    offset = jax.random.uniform(subkeys[5], (1, NVOX), jnp.float32, -5.0, 5.0)
    noise_part = jax.random.normal(subkeys[2], (TRS, NVOX), jnp.float32)
    vox_scale = jnp.exp(jax.random.uniform(subkeys[3], (1, NVOX), jnp.float32, 0.0, math.log(10.0)))
    signal = jnp.dot(latent, loadings) + noise_part
    return (offset + vox_scale * tr_scale * signal).astype(jnp.float32)


def routing(key):
    base_key = jax.random.fold_in(key, 7)
    row_blocks = NTILES // RT
    col_blocks = NTILES // CT
    owner_order = jax.random.permutation(jax.random.fold_in(base_key, 1), row_blocks)
    shifts = jax.vmap(lambda subkey: jax.random.permutation(subkey, RT))(jax.random.split(jax.random.fold_in(base_key, 2), row_blocks))
    block_ids = jnp.arange(row_blocks, dtype=jnp.int32)[:, None]
    owners = owner_order[(block_ids + shifts) % row_blocks].reshape(NTILES).astype(jnp.int32)
    load_level = jax.random.randint(jax.random.fold_in(base_key, 3), (row_blocks,), 0, 3)
    slot_draw = jax.random.randint(jax.random.fold_in(base_key, 4), (NTILES, col_blocks), 0, CAP + 1)
    slot_limit = jnp.minimum(CAP, slot_draw * (1 + load_level[owners])[:, None] // 2)
    forced = (owners == owner_order[0])[:, None] & (jnp.arange(col_blocks) == 0)[None, :]
    slot_limit = jnp.where(forced, CAP, slot_limit)
    tile_ranks = jax.vmap(lambda subkey: jax.random.permutation(subkey, CT))(jax.random.split(jax.random.fold_in(base_key, 5), NTILES * col_blocks))
    tile_ranks = tile_ranks.reshape(NTILES, col_blocks, CT)
    kept = (tile_ranks < slot_limit[:, :, None]).astype(jnp.int32).reshape(NTILES, NTILES)
    return (kept, owners)


def draw_keep_mask(key, part):
    kept, owners = routing(key)
    return kept


def draw_row_owner(key, part):
    kept, owners = routing(key)
    return owners


def setup_inputs(seed: int = 0, part: int = 0) -> dict:
    key_of = jax.random.split(jax.random.key(seed), 4)
    part_keys = jax.random.split(jax.random.fold_in(key_of[3], part), 4)
    series = draw_series(jax.random.fold_in(jax.random.fold_in(key_of[3], part), 71), part)
    keep_mask = draw_keep_mask(jax.random.fold_in(jax.random.fold_in(key_of[3], part), 71), part)
    row_owner = draw_row_owner(jax.random.fold_in(jax.random.fold_in(key_of[3], part), 71), part)
    return {"series": series, "keep_mask": keep_mask, "row_owner": row_owner}


epsilon = 1e-05

def reference(series, keep_mask, row_owner):
    average = lax.optimization_barrier(jnp.mean(series, axis=0, keepdims=True))
    centred = series - average
    spread = lax.optimization_barrier(jnp.mean(centred * centred, axis=0, keepdims=True))
    scored = (centred * lax.rsqrt(spread + epsilon)).astype(jnp.bfloat16)
    reordered = scored.reshape(TRS, N_ROW, N_COL, CH).transpose(0, 2, 1, 3).reshape(TRS, NVOX)
    row_tiles = scored.reshape(TRS, NTILES, TILE)
    col_tiles = reordered.reshape(TRS, NTILES, TILE)
    positions = jnp.arange(NTILES * CT, dtype=jnp.int32)
    slot_index = jnp.arange(RCAP, dtype=jnp.int32)

    def one_group(group_index):
        target = group_index // N_COL
        column_block = group_index % N_COL
        block_keep = lax.dynamic_slice_in_dim(keep_mask, (column_block * CT).astype(jnp.int32), CT, 1)
        owned = (row_owner == target).astype(jnp.int32)
        keep_flags = (block_keep * owned[:, None]).reshape(NTILES * CT)
        running = jnp.cumsum(keep_flags)
        slot_hit = (keep_flags[None, :] == 1) & (running[None, :] == slot_index[:, None] + 1)
        picked = lax.optimization_barrier(jnp.sum(jnp.where(slot_hit, positions[None, :], 0), axis=1)).astype(jnp.int32)
        present = running[-1] > slot_index
        row_ids = (picked // CT).astype(jnp.int32)
        col_ids = (column_block * CT + picked % CT).astype(jnp.int32)
        left_tiles = jnp.take(row_tiles, row_ids, axis=1).astype(jnp.float32)
        right_tiles = jnp.take(col_tiles, col_ids, axis=1).astype(jnp.float32)
        products = jnp.einsum('tsa,tsb->sab', left_tiles, right_tiles) * (1.0 / TRS)
        slot_tiles = jnp.where(present[:, None, None], products, 0.0).astype(jnp.bfloat16)
        slot_ids = jnp.where(present, row_ids * NTILES + col_ids, -1).astype(jnp.int32)
        return (slot_tiles, slot_ids)
    slot_tiles, slot_ids = lax.map(one_group, jnp.arange(N_ROW * N_COL, dtype=jnp.int32))
    return (slot_tiles.reshape(N_ROW, N_COL, RCAP, TILE, TILE), slot_ids.reshape(N_ROW, N_COL, RCAP))
```

```python
import functools

import jax
import jax.numpy as jnp
from jax import lax
from jax.experimental import pallas as pl
from jax.experimental.pallas import tpu as pltpu
from jax.sharding import PartitionSpec as P

TILE = 128
EPSILON = 1e-05
MESH = pl.DeviceIdType.MESH


PIECES = 4


def peers(n_row, r):
    if n_row % 2:
        return [lax.rem(r + k, n_row) for k in range(1, n_row)]
    chips = n_row // 2
    pairs = [(i, j) for i in range(1, chips) for j in range(2)] + [(0, 1)]
    return [
        lax.rem(lax.div(r, 2) + i, chips) * 2 + lax.rem(lax.rem(r, 2) + j, 2) for i, j in pairs
    ]


def kernel(
    n_row,
    n_col,
    series_hbm,
    keep_hbm,
    owner_hbm,
    packed,
    ids_out,
    series,
    keep_smem,
    keep_vmem,
    owner_smem,
    row_main,
    row_rest,
    rest_part,
    col_block,
    grid,
    outbox,
    inbox,
    plan,
    keep_all,
    keep_all_smem,
    load_sem,
    small_sem,
    keep_sem,
    z_send,
    z_recv,
    x_send,
    x_recv,
    t_send,
    t_recv,
    m_send,
    m_recv,
):
    frames = series.shape[0]
    rt, ct = keep_smem.shape
    cap = outbox.shape[1]
    slots = packed.shape[0]
    main = row_main.shape[2]
    rest = frames - main
    step = TILE // PIECES
    order = ([PIECES] if rest else []) + list(range(PIECES))
    r = lax.axis_index("row")
    c = lax.axis_index("col")
    others = peers(n_row, r)
    has_left = c > 0
    has_right = c < n_col - 1

    load = pltpu.make_async_copy(series_hbm, series, load_sem)
    load.start()
    small = [
        pltpu.make_async_copy(keep_hbm, keep_vmem, small_sem.at[0]),
        pltpu.make_async_copy(keep_hbm, keep_smem, small_sem.at[1]),
        pltpu.make_async_copy(owner_hbm, owner_smem, small_sem.at[2]),
    ]
    for copy in small:
        copy.start()

    barrier = pltpu.get_barrier_semaphore()
    for other in others:
        pl.semaphore_signal(barrier, inc=1, device_id={"row": other}, device_id_type=MESH)

    @pl.when(has_left)
    def _():
        pl.semaphore_signal(barrier, inc=1, device_id={"col": c - 1}, device_id_type=MESH)

    @pl.when(has_right)
    def _():
        pl.semaphore_signal(barrier, inc=1, device_id={"col": c + 1}, device_id_type=MESH)

    for copy in small:
        copy.wait()
    load.wait()
    values = series[...]
    average = jnp.sum(values, axis=0, keepdims=True) * (1.0 / frames)
    centred = values - average
    spread = jnp.sum(centred * centred, axis=0, keepdims=True) * (1.0 / frames)
    scale = lax.rsqrt(spread + EPSILON)

    pl.semaphore_wait(
        barrier, n_row - 1 + has_left.astype(jnp.int32) + has_right.astype(jnp.int32)
    )

    def z_copy(shard, chunk, side, target):
        if chunk == PIECES:
            part = row_rest.at[shard]
        else:
            part = row_main.at[shard, pl.ds(chunk * step, step), :]
        return pltpu.make_async_remote_copy(
            src_ref=part,
            dst_ref=part,
            send_sem=z_send.at[side, shard, chunk],
            recv_sem=z_recv.at[shard, chunk],
            device_id={"col": target},
            device_id_type=MESH,
        )

    def to_right(shard, chunk):
        return z_copy(shard, chunk, 0, c + 1)

    def to_left(shard, chunk):
        return z_copy(shard, chunk, 1, c - 1)

    def row_copy(k, src, dst, send, recv):
        return pltpu.make_async_remote_copy(
            src_ref=src,
            dst_ref=dst,
            send_sem=send,
            recv_sem=recv,
            device_id={"row": others[k]},
            device_id_type=MESH,
        )

    def mask_copy(k):
        return row_copy(k, keep_vmem, keep_all.at[r], m_send.at[k], m_recv.at[k])

    def scored_copy(k):
        return row_copy(k, col_block.at[r], col_block.at[r], x_send.at[k], x_recv.at[k])

    def tile_copy(k, v):
        part = pl.ds(v * step, step)
        return row_copy(
            k,
            outbox.at[k, :, part, :],
            inbox.at[pl.ds(r * cap, cap), part, :],
            t_send.at[k, v],
            t_recv.at[k, v],
        )

    peer_range = range(n_row - 1)
    for k in peer_range:
        mask_copy(k).start()
    keep_all[r] = keep_vmem[...]

    scored = centred * scale
    if rest:
        row_rest[c] = scored[main:].astype(jnp.bfloat16)
    flipped = jnp.transpose(scored[:main]).astype(jnp.bfloat16)
    row_main[c] = flipped

    for j in order:

        @pl.when(has_right)
        def _():
            to_right(c, j).start()

        @pl.when(has_left)
        def _():
            to_left(c, j).start()

    col_block[r] = scored.astype(jnp.bfloat16)
    for k in peer_range:
        scored_copy(k).start()

    width = 2 if n_row % 2 == 0 else 1

    def over_columns(body):
        if n_row <= 4:
            for p in range(n_row // width):
                body(p)
        else:

            def step_body(p, carry):
                body(p)
                return carry

            lax.fori_loop(0, n_row // width, step_body, 0)

    def columns(p, part):
        return jnp.concatenate([col_block[p * width + w, part, :] for w in range(width)], axis=1)

    def dot(left, right, axis):
        return lax.dot_general(
            left, right, (((axis,), (0,)), ((), ())), preferred_element_type=jnp.float32
        )

    def multiply_rest(m):
        def body(p):
            rest_part[p] = dot(row_rest[m], columns(p, pl.ds(main, rest)), 0)

        if rest:
            over_columns(body)

    def multiply_rows(m, rows):
        def body(p):
            product = dot(row_main[m, rows, :], columns(p, pl.ds(0, main)), 1)
            if rest:
                product = product + rest_part[p, rows, :]
            product = (product * (1.0 / frames)).astype(jnp.bfloat16)
            for w in range(width):
                grid[m, p * width + w, rows, :] = product[:, w * TILE : (w + 1) * TILE]

        over_columns(body)

    def multiply(m):
        multiply_rest(m)
        multiply_rows(m, pl.ds(0, TILE))

    def pack_plan():
        keep_copy = pltpu.make_async_copy(keep_all, keep_all_smem, keep_sem)
        keep_copy.start()
        keep_copy.wait()
        lanes = lax.broadcasted_iota(jnp.int32, (1, slots), 1)
        ids = jnp.full((1, slots), -1, jnp.int32)
        total = jnp.int32(0)
        starts = []
        for b in range(n_row):
            line = jnp.int32(0)
            for i in range(rt):
                line = jnp.where(owner_smem[b * rt + i] == r, i, line)
            starts.append(total)
            for j in range(ct):
                kept = keep_all_smem[b, line, j]
                name = (b * rt + line) * (ct * n_col) + c * ct + j
                ids = jnp.where((lanes == total) & (kept == 1), name, ids)
                total = total + kept
        ids_out[...] = ids
        for s in range(slots):
            source = jnp.int32(s)
            for b in range(1, n_row):
                source = jnp.where(s >= starts[b], b * cap + s - starts[b], source)
            plan[s] = jnp.where(s < total, source, n_row * cap)
        inbox[n_row * cap] = jnp.zeros((TILE, TILE), jnp.bfloat16)

    def choose(target):
        line = jnp.int32(0)
        for i in range(rt):
            line = jnp.where(owner_smem[r * rt + i] == target, i, line)
        picks = [jnp.int32(0)] * cap
        count = jnp.int32(0)
        for j in range(ct):
            kept = keep_smem[line, j]
            for s in range(cap):
                picks[s] = jnp.where((kept == 1) & (count == s), j, picks[s])
            count = count + kept
        return line, picks

    for hop in range(1, n_col - 1):
        for j in order:

            @pl.when(c - hop >= 0)
            def _():
                to_right(c - hop, j).wait_recv()

                @pl.when(has_right)
                def _():
                    to_right(c - hop, j).start()

            @pl.when(c + hop < n_col)
            def _():
                to_left(c + hop, j).wait_recv()

                @pl.when(has_left)
                def _():
                    to_left(c + hop, j).start()

    for k in peer_range:
        mask_copy(k).wait_recv()
    pack_plan()
    choices = [choose(target) for target in others + [r]]
    for k in peer_range:
        scored_copy(k).wait_recv()
    multiply(c)
    for near in range(1, n_col - 1):

        @pl.when(c - near >= 0)
        def _():
            multiply(c - near)

        @pl.when(c + near < n_col)
        def _():
            multiply(c + near)

    last = n_col - 1
    for j in order:
        if last:

            @pl.when(c == last)
            def _():
                to_right(0, j).wait_recv()
                if j == PIECES:
                    multiply_rest(0)
                else:
                    multiply_rows(0, pl.ds(j * step, step))

            @pl.when(c == 0)
            def _():
                to_left(last, j).wait_recv()
                if j == PIECES:
                    multiply_rest(last)
                else:
                    multiply_rows(last, pl.ds(j * step, step))

        if j == PIECES:
            continue
        rows = pl.ds(j * step, step)
        for k in peer_range:
            line, picks = choices[k]
            for s in range(cap):
                outbox[k, s, rows, :] = grid[line, picks[s], rows, :]
            tile_copy(k, j).start()
        line, picks = choices[-1]
        for s in range(cap):
            inbox[r * cap + s, rows, :] = grid[line, picks[s], rows, :]

    for j in order:
        for hop in range(n_col):

            @pl.when((c - hop >= 0) & has_right)
            def _():
                to_right(c - hop, j).wait_send()

            @pl.when((c + hop < n_col) & has_left)
            def _():
                to_left(c + hop, j).wait_send()

    for k in peer_range:
        mask_copy(k).wait_send()
        scored_copy(k).wait_send()
        for v in range(PIECES):
            tile_copy(k, v).wait()

    if slots <= 8:
        for s in range(slots):
            packed[s] = inbox[plan[s]]
    else:

        def pack_slot(s, carry):
            packed[s] = inbox[plan[s]]
            return carry

        lax.fori_loop(0, slots, pack_slot, 0)


def write(tiles, ids, tiles_out, ids_out, sems):
    copies = [
        pltpu.make_async_copy(tiles, tiles_out, sems.at[0]),
        pltpu.make_async_copy(ids, ids_out, sems.at[1]),
    ]
    for copy in copies:
        copy.start()
    for copy in copies:
        copy.wait()


def shards(n_row, n_col, series, keep_mask, row_owner):
    frames = series.shape[0]
    rt, ct = keep_mask.shape
    cap = max(2, 3 * ct // 8)
    slots = rt * cap
    main = frames // TILE * TILE
    rest = max(frames - main, 16)
    links = max(n_row - 1, 1)
    width = 2 if n_row % 2 == 0 else 1
    dma = pltpu.SemaphoreType.DMA
    vmem = pl.BlockSpec(memory_space=pltpu.VMEM)
    hbm = pl.BlockSpec(memory_space=pltpu.HBM)
    packed, ids = pl.pallas_call(
        functools.partial(kernel, n_row, n_col),
        out_shape=(
            jax.ShapeDtypeStruct((slots, TILE, TILE), jnp.bfloat16),
            jax.ShapeDtypeStruct((1, slots), jnp.int32),
        ),
        in_specs=[hbm, hbm, hbm],
        out_specs=(vmem, vmem),
        scratch_shapes=[
            pltpu.VMEM((frames, TILE), jnp.float32),
            pltpu.SMEM((rt, ct), jnp.int32),
            pltpu.VMEM((rt, ct), jnp.int32),
            pltpu.SMEM(row_owner.shape, jnp.int32),
            pltpu.VMEM((n_col, TILE, main), jnp.bfloat16),
            pltpu.VMEM((n_col, rest, TILE), jnp.bfloat16),
            pltpu.VMEM((n_row // width, TILE, width * TILE), jnp.float32),
            pltpu.VMEM((n_row, frames, TILE), jnp.bfloat16),
            pltpu.VMEM((rt, ct, TILE, TILE), jnp.bfloat16),
            pltpu.VMEM((links, cap, TILE, TILE), jnp.bfloat16),
            pltpu.VMEM((n_row * cap + 1, TILE, TILE), jnp.bfloat16),
            pltpu.SMEM((slots,), jnp.int32),
            pltpu.VMEM((n_row, rt, ct), jnp.int32),
            pltpu.SMEM((n_row, rt, ct), jnp.int32),
            dma(()),
            dma((3,)),
            dma(()),
            dma((2, n_col, PIECES + 1)),
            dma((n_col, PIECES + 1)),
            dma((links,)),
            dma((links,)),
            dma((links, PIECES)),
            dma((links, PIECES)),
            dma((links,)),
            dma((links,)),
        ],
        compiler_params=pltpu.CompilerParams(
            collective_id=0, has_side_effects=True, vmem_limit_bytes=32 * 1024 * 1024
        ),
    )(*(pltpu.with_memory_space_constraint(x, pltpu.HBM) for x in (series, keep_mask, row_owner)))
    tiles, ids = pl.pallas_call(
        write,
        out_shape=(
            jax.ShapeDtypeStruct((slots, TILE, TILE), jnp.bfloat16),
            jax.ShapeDtypeStruct((1, slots), jnp.int32),
        ),
        in_specs=[vmem, vmem],
        out_specs=(hbm, hbm),
        scratch_shapes=[dma((2,))],
        compiler_params=pltpu.CompilerParams(vmem_limit_bytes=16 * 1024 * 1024),
    )(packed, ids)
    return tiles.reshape(1, 1, slots, TILE, TILE), ids.reshape(1, 1, slots)


def solution(mesh):
    in_specs = (P(None, ("subj", "row", "col")), P(("subj", "row"), "col"), P("subj"))
    out_specs = (P(("subj", "row"), "col", None, None, None), P(("subj", "row"), "col", None))
    return jax.shard_map(
        functools.partial(shards, mesh.shape["row"], mesh.shape["col"]),
        mesh=mesh,
        in_specs=in_specs,
        out_specs=out_specs,
        check_vma=False,
    )
```

```python
import functools

import jax
import jax.numpy as jnp
from jax import lax
from jax.experimental import pallas as pl
from jax.experimental.pallas import tpu as pltpu
from jax.sharding import PartitionSpec as P

TILE = 128
EPSILON = 1e-05
MESH = pl.DeviceIdType.MESH


LOADS = 8
SIZES = (64, 32, 32)
PIECES = len(SIZES)
PARTS = [pl.ds(sum(SIZES[:i]), size) for i, size in enumerate(SIZES)]


def peers(n_row, r):
    if n_row % 2:
        return [lax.rem(r + k, n_row) for k in range(1, n_row)]
    chips = n_row // 2
    pairs = [(i, j) for i in range(1, chips) for j in range(2)] + [(0, 1)]
    return [
        lax.rem(lax.div(r, 2) + i, chips) * 2 + lax.rem(lax.rem(r, 2) + j, 2) for i, j in pairs
    ]


def kernel(
    n_row,
    n_col,
    series_hbm,
    keep_hbm,
    owner_hbm,
    packed,
    ids_out,
    series,
    keep_smem,
    keep_vmem,
    owner_smem,
    row_main,
    row_rest,
    rest_part,
    col_block,
    grid,
    outbox,
    inbox,
    plan,
    keep_all,
    keep_all_smem,
    right_sem,
    load_sem,
    small_sem,
    keep_sem,
    z_send,
    z_recv,
    x_send,
    x_recv,
    t_send,
    t_recv,
    m_send,
    m_recv,
):
    frames = series.shape[0]
    rt, ct = keep_smem.shape
    cap = outbox.shape[1]
    slots = packed.shape[0]
    main = row_main.shape[2]
    rest = frames - main
    order = ([PIECES] if rest else []) + list(range(PIECES))
    r = lax.axis_index("row")
    c = lax.axis_index("col")
    others = peers(n_row, r)
    has_left = c > 0
    has_right = c < n_col - 1

    cuts = [frames * i // LOADS // 8 * 8 for i in range(LOADS)] + [frames]
    loads = [
        pltpu.make_async_copy(
            series_hbm.at[pl.ds(low, high - low), :],
            series.at[pl.ds(low, high - low), :],
            load_sem.at[i],
        )
        for i, (low, high) in enumerate(zip(cuts[:-1], cuts[1:]))
    ]
    for load in loads:
        load.start()
    small = [
        pltpu.make_async_copy(keep_hbm, keep_vmem, small_sem.at[0]),
        pltpu.make_async_copy(keep_hbm, keep_smem, small_sem.at[1]),
        pltpu.make_async_copy(owner_hbm, owner_smem, small_sem.at[2]),
    ]
    for copy in small:
        copy.start()

    barrier = pltpu.get_barrier_semaphore()
    for other in others:
        pl.semaphore_signal(barrier, inc=1, device_id={"row": other}, device_id_type=MESH)

    @pl.when(has_right)
    def _():
        pl.semaphore_signal(barrier, inc=1, device_id={"col": c + 1}, device_id_type=MESH)

    for copy in small:
        copy.wait()
    total = jnp.zeros((8, TILE), jnp.float32)
    for load, low, high in zip(loads, cuts[:-1], cuts[1:]):
        load.wait()
        total = total + jnp.sum(series[low:high, :].reshape(-1, 8, TILE), axis=0)
    average = jnp.sum(total, axis=0, keepdims=True) * (1.0 / frames)
    values = series[...]
    centred = values - average
    spread = jnp.sum(centred * centred, axis=0, keepdims=True) * (1.0 / frames)
    scale = lax.rsqrt(spread + EPSILON)

    pl.semaphore_wait(barrier, n_row - 1 + has_left.astype(jnp.int32))

    @pl.when(has_left)
    def _():
        pl.semaphore_signal(right_sem, inc=1, device_id={"col": c - 1}, device_id_type=MESH)

    def z_copy(shard, chunk, side, target):
        if chunk == PIECES:
            part = row_rest.at[shard]
        else:
            part = row_main.at[shard, PARTS[chunk], :]
        return pltpu.make_async_remote_copy(
            src_ref=part,
            dst_ref=part,
            send_sem=z_send.at[side, shard, chunk],
            recv_sem=z_recv.at[shard, chunk],
            device_id={"col": target},
            device_id_type=MESH,
        )

    def to_right(shard, chunk):
        return z_copy(shard, chunk, 0, c + 1)

    def to_left(shard, chunk):
        return z_copy(shard, chunk, 1, c - 1)

    def row_copy(k, src, dst, send, recv):
        return pltpu.make_async_remote_copy(
            src_ref=src,
            dst_ref=dst,
            send_sem=send,
            recv_sem=recv,
            device_id={"row": others[k]},
            device_id_type=MESH,
        )

    def mask_copy(k):
        return row_copy(k, keep_vmem, keep_all.at[r], m_send.at[k], m_recv.at[k])

    def scored_copy(k):
        return row_copy(k, col_block.at[r], col_block.at[r], x_send.at[k], x_recv.at[k])

    def tile_copy(k, v):
        part = PARTS[v]
        return row_copy(
            k,
            outbox.at[k, :, part, :],
            inbox.at[pl.ds(r * cap, cap), part, :],
            t_send.at[k, v],
            t_recv.at[k, v],
        )

    peer_range = range(n_row - 1)
    for k in peer_range:
        mask_copy(k).start()
    keep_all[r] = keep_vmem[...]

    scored = centred * scale
    if rest:
        row_rest[c] = scored[main:].astype(jnp.bfloat16)
    flipped = jnp.transpose(scored[:main]).astype(jnp.bfloat16)
    row_main[c] = flipped

    for j in order:

        @pl.when(has_left)
        def _():
            to_left(c, j).start()

    col_block[r] = scored.astype(jnp.bfloat16)
    for k in peer_range:
        scored_copy(k).start()

    @pl.when(has_right)
    def _():
        pl.semaphore_wait(right_sem, 1)
        for j in order:
            to_right(c, j).start()

    width = 2 if n_row % 2 == 0 else 1

    def over_columns(body):
        if n_row <= 4:
            for p in range(n_row // width):
                body(p)
        else:

            def step_body(p, carry):
                body(p)
                return carry

            lax.fori_loop(0, n_row // width, step_body, 0)

    def columns(p, part):
        return jnp.concatenate([col_block[p * width + w, part, :] for w in range(width)], axis=1)

    def dot(left, right, axis):
        return lax.dot_general(
            left, right, (((axis,), (0,)), ((), ())), preferred_element_type=jnp.float32
        )

    def multiply_rest(m):
        def body(p):
            rest_part[p] = dot(row_rest[m], columns(p, pl.ds(main, rest)), 0)

        if rest:
            over_columns(body)

    def multiply_rows(m, rows):
        def body(p):
            product = dot(row_main[m, rows, :], columns(p, pl.ds(0, main)), 1)
            if rest:
                product = product + rest_part[p, rows, :]
            product = (product * (1.0 / frames)).astype(jnp.bfloat16)
            for w in range(width):
                grid[m, p * width + w, rows, :] = product[:, w * TILE : (w + 1) * TILE]

        over_columns(body)

    def multiply(m):
        multiply_rest(m)
        multiply_rows(m, pl.ds(0, TILE))

    def pack_plan():
        keep_copy = pltpu.make_async_copy(keep_all, keep_all_smem, keep_sem)
        keep_copy.start()
        keep_copy.wait()
        lanes = lax.broadcasted_iota(jnp.int32, (1, slots), 1)
        ids = jnp.full((1, slots), -1, jnp.int32)
        total = jnp.int32(0)
        starts = []
        for b in range(n_row):
            line = jnp.int32(0)
            for i in range(rt):
                line = jnp.where(owner_smem[b * rt + i] == r, i, line)
            starts.append(total)
            for j in range(ct):
                kept = keep_all_smem[b, line, j]
                name = (b * rt + line) * (ct * n_col) + c * ct + j
                ids = jnp.where((lanes == total) & (kept == 1), name, ids)
                total = total + kept
        ids_out[...] = ids
        for s in range(slots):
            source = jnp.int32(s)
            for b in range(1, n_row):
                source = jnp.where(s >= starts[b], b * cap + s - starts[b], source)
            plan[s] = jnp.where(s < total, source, n_row * cap)
        inbox[n_row * cap] = jnp.zeros((TILE, TILE), jnp.bfloat16)

    def choose(target):
        line = jnp.int32(0)
        for i in range(rt):
            line = jnp.where(owner_smem[r * rt + i] == target, i, line)
        picks = [jnp.int32(0)] * cap
        count = jnp.int32(0)
        for j in range(ct):
            kept = keep_smem[line, j]
            for s in range(cap):
                picks[s] = jnp.where((kept == 1) & (count == s), j, picks[s])
            count = count + kept
        return line, picks

    for hop in range(1, n_col - 1):
        for j in order:

            @pl.when(c + hop < n_col)
            def _():
                to_left(c + hop, j).wait_recv()

                @pl.when(has_left)
                def _():
                    to_left(c + hop, j).start()

            @pl.when(c - hop >= 0)
            def _():
                to_right(c - hop, j).wait_recv()

                @pl.when(has_right)
                def _():
                    to_right(c - hop, j).start()

    for k in peer_range:
        mask_copy(k).wait_recv()
    pack_plan()
    choices = [choose(target) for target in others + [r]]
    for k in peer_range:
        scored_copy(k).wait_recv()
    multiply(c)
    for near in range(1, n_col - 1):

        @pl.when(c - near >= 0)
        def _():
            multiply(c - near)

        @pl.when(c + near < n_col)
        def _():
            multiply(c + near)

    last = n_col - 1
    for j in order:
        if last:

            @pl.when(c == last)
            def _():
                to_right(0, j).wait_recv()
                if j == PIECES:
                    multiply_rest(0)
                else:
                    multiply_rows(0, PARTS[j])

            @pl.when(c == 0)
            def _():
                to_left(last, j).wait_recv()
                if j == PIECES:
                    multiply_rest(last)
                else:
                    multiply_rows(last, PARTS[j])

        if j == PIECES:
            continue
        rows = PARTS[j]
        for k in peer_range:
            line, picks = choices[k]
            for s in range(cap):
                outbox[k, s, rows, :] = grid[line, picks[s], rows, :]
            tile_copy(k, j).start()
        line, picks = choices[-1]
        for s in range(cap):
            inbox[r * cap + s, rows, :] = grid[line, picks[s], rows, :]

    for j in order:
        for hop in range(n_col):

            @pl.when((c - hop >= 0) & has_right)
            def _():
                to_right(c - hop, j).wait_send()

            @pl.when((c + hop < n_col) & has_left)
            def _():
                to_left(c + hop, j).wait_send()

    for k in peer_range:
        mask_copy(k).wait_send()
        scored_copy(k).wait_send()
        for v in range(PIECES):
            tile_copy(k, v).wait()

    if slots <= 8:
        for s in range(slots):
            packed[s] = inbox[plan[s]]
    else:

        def pack_slot(s, carry):
            packed[s] = inbox[plan[s]]
            return carry

        lax.fori_loop(0, slots, pack_slot, 0)


def write(tiles, ids, tiles_out, ids_out, sems):
    copies = [
        pltpu.make_async_copy(tiles, tiles_out, sems.at[0]),
        pltpu.make_async_copy(ids, ids_out, sems.at[1]),
    ]
    for copy in copies:
        copy.start()
    for copy in copies:
        copy.wait()


def shards(n_row, n_col, series, keep_mask, row_owner):
    frames = series.shape[0]
    rt, ct = keep_mask.shape
    cap = max(2, 3 * ct // 8)
    slots = rt * cap
    main = frames // TILE * TILE
    rest = max(frames - main, 16)
    links = max(n_row - 1, 1)
    width = 2 if n_row % 2 == 0 else 1
    dma = pltpu.SemaphoreType.DMA
    vmem = pl.BlockSpec(memory_space=pltpu.VMEM)
    hbm = pl.BlockSpec(memory_space=pltpu.HBM)
    packed, ids = pl.pallas_call(
        functools.partial(kernel, n_row, n_col),
        out_shape=(
            jax.ShapeDtypeStruct((slots, TILE, TILE), jnp.bfloat16),
            jax.ShapeDtypeStruct((1, slots), jnp.int32),
        ),
        in_specs=[hbm, hbm, hbm],
        out_specs=(vmem, vmem),
        scratch_shapes=[
            pltpu.VMEM((frames, TILE), jnp.float32),
            pltpu.SMEM((rt, ct), jnp.int32),
            pltpu.VMEM((rt, ct), jnp.int32),
            pltpu.SMEM(row_owner.shape, jnp.int32),
            pltpu.VMEM((n_col, TILE, main), jnp.bfloat16),
            pltpu.VMEM((n_col, rest, TILE), jnp.bfloat16),
            pltpu.VMEM((n_row // width, TILE, width * TILE), jnp.float32),
            pltpu.VMEM((n_row, frames, TILE), jnp.bfloat16),
            pltpu.VMEM((rt, ct, TILE, TILE), jnp.bfloat16),
            pltpu.VMEM((links, cap, TILE, TILE), jnp.bfloat16),
            pltpu.VMEM((n_row * cap + 1, TILE, TILE), jnp.bfloat16),
            pltpu.SMEM((slots,), jnp.int32),
            pltpu.VMEM((n_row, rt, ct), jnp.int32),
            pltpu.SMEM((n_row, rt, ct), jnp.int32),
            pltpu.SemaphoreType.REGULAR,
            dma((LOADS,)),
            dma((3,)),
            dma(()),
            dma((2, n_col, PIECES + 1)),
            dma((n_col, PIECES + 1)),
            dma((links,)),
            dma((links,)),
            dma((links, PIECES)),
            dma((links, PIECES)),
            dma((links,)),
            dma((links,)),
        ],
        compiler_params=pltpu.CompilerParams(
            collective_id=0, has_side_effects=True, vmem_limit_bytes=32 * 1024 * 1024
        ),
    )(*(pltpu.with_memory_space_constraint(x, pltpu.HBM) for x in (series, keep_mask, row_owner)))
    tiles, ids = pl.pallas_call(
        write,
        out_shape=(
            jax.ShapeDtypeStruct((slots, TILE, TILE), jnp.bfloat16),
            jax.ShapeDtypeStruct((1, slots), jnp.int32),
        ),
        in_specs=[vmem, vmem],
        out_specs=(hbm, hbm),
        scratch_shapes=[dma((2,))],
        compiler_params=pltpu.CompilerParams(vmem_limit_bytes=16 * 1024 * 1024),
    )(packed, ids)
    return tiles.reshape(1, 1, slots, TILE, TILE), ids.reshape(1, 1, slots)


def solution(mesh):
    in_specs = (P(None, ("subj", "row", "col")), P(("subj", "row"), "col"), P("subj"))
    out_specs = (P(("subj", "row"), "col", None, None, None), P(("subj", "row"), "col", None))
    return jax.shard_map(
        functools.partial(shards, mesh.shape["row"], mesh.shape["col"]),
        mesh=mesh,
        in_specs=in_specs,
        out_specs=out_specs,
        check_vma=False,
    )
```
